8 devices in a mesh: grp: 1 (over z), dz: 2 (over y), dy: 2 (over x), dx: 2 (over core).
Axes of the slice: x: 2, y: 2, z: 1, core: 2. Of those that a mesh axis runs over, the one named last changes fastest.
Arguments:
- x_in: bfloat16 [8192, 7168], P(('grp', 'dx', 'dz'), 'dy')
- w_gate: bfloat16 [7168, 20480], P('dy', ('dz', 'dx'))
- w_up: bfloat16 [7168, 20480], P('dy', ('dz', 'dx'))
- w_down: bfloat16 [20480, 7168], P('dz', ('dy', 'dx'))
Outputs:
- output: bfloat16 [8192, 7168], P(('grp', 'dx', 'dz'), 'dy')
All inputs are finite; a program needn't handle non-finite values.
Results may differ from the reference program's by a relative error of at most 0.0124753.
Values are sent between devices in bfloat16 or wider.
A program may use at most 1 GiB of HBM per device.

```python
import jax
import jax.numpy as jnp
from jax import lax

N_ROWS = 8192
D_MODEL = 7168
D_FF = 20480
ROW_TILE = 2048


def setup_inputs(seed: int = 0, part: int = 0) -> dict:
    base_key = jax.random.key(seed)
    key_x = jax.random.fold_in(jax.random.fold_in(base_key, 1), part)
    key_gate = jax.random.fold_in(base_key, 2)
    key_up = jax.random.fold_in(base_key, 3)
    key_down = jax.random.fold_in(base_key, 4)
    x_in = jax.random.normal(key_x, (N_ROWS, D_MODEL), jnp.float32).astype(jnp.bfloat16)
    w_gate = (jax.random.normal(key_gate, (D_MODEL, D_FF), jnp.float32) * D_MODEL ** -0.5).astype(jnp.bfloat16)
    w_up = (jax.random.normal(key_up, (D_MODEL, D_FF), jnp.float32) * D_MODEL ** -0.5).astype(jnp.bfloat16)
    w_down = (jax.random.normal(key_down, (D_FF, D_MODEL), jnp.float32) * D_FF ** -0.5).astype(jnp.bfloat16)
    return {"x_in": x_in, "w_gate": w_gate, "w_up": w_up, "w_down": w_down}


def reference(x_in, w_gate, w_up, w_down):
    def row_tile(x_tile):
        gate_val = jnp.dot(x_tile, w_gate, preferred_element_type=jnp.float32).astype(jnp.bfloat16)
        up_val = jnp.dot(x_tile, w_up, preferred_element_type=jnp.float32).astype(jnp.bfloat16)
        hidden = (jax.nn.silu(gate_val.astype(jnp.float32)) * up_val.astype(jnp.float32)).astype(jnp.bfloat16)
        return jnp.dot(hidden, w_down, preferred_element_type=jnp.float32).astype(jnp.bfloat16)
    x_tiles = x_in.reshape(N_ROWS // ROW_TILE, ROW_TILE, D_MODEL)
    return lax.map(row_tile, x_tiles).reshape(N_ROWS, D_MODEL)
```

```python
import jax
import jax.numpy as jnp
from jax import lax
from jax.sharding import PartitionSpec as P


CHUNKS = 4


def solution(mesh):
    x_spec = P(("grp", "dx", "dz"), "dy")
    w_in_spec = P("dy", ("dz", "dx"))
    w_out_spec = P("dz", ("dy", "dx"))

    def swap(arr, axis):
        return lax.ppermute(arr, axis, [(0, 1), (1, 0)])

    def dot(lhs, rhs):
        return jnp.dot(lhs, rhs, preferred_element_type=jnp.float32)

    def body(x_blk, wg_blk, wu_blk, wd_blk):
        my_y = lax.axis_index("dy")
        my_c = lax.axis_index("dx")
        rows = x_blk.shape[0] // CHUNKS
        cols = wg_blk.shape[1] // 2
        n = 2 * CHUNKS

        def half(w_blk, which):
            return lax.dynamic_slice_in_dim(w_blk, which * cols, cols, axis=1)

        x_own = [x_blk[i * rows:(i + 1) * rows] for i in range(CHUNKS)]
        x_own_far = [swap(x_own[i], "dy") for i in range(CHUNKS)]
        x_oth = swap(x_blk, "dz")
        x_oth_far = [swap(x_own_far[i], "dz") for i in range(CHUNKS)]
        g_far = swap(half(wg_blk, 1 - my_y), "dy")
        u_far = swap(half(wu_blk, 1 - my_y), "dy")
        g_near = half(wg_blk, my_y)
        u_near = half(wu_blk, my_y)
        g_near = [g_near, swap(g_near, "dx")]
        u_near = [u_near, swap(u_near, "dx")]
        g_far = [g_far, swap(g_far, "dx")]
        u_far = [u_far, swap(u_far, "dx")]

        wd_all = lax.all_gather(wd_blk, "dx", axis=1, tiled=True)
        wd4 = wd_all.reshape(2, 2, cols, wd_all.shape[1])
        wd4 = jnp.where(my_c == 1, lax.rev(wd4, (0,)), wd4)
        wd4 = jnp.where(my_y == 1, lax.rev(wd4, (1,)), wd4)
        wd_perm = wd4.reshape(wd_all.shape)

        far = x_oth_far + x_own_far
        parts = {}
        for s, near in (("o", x_oth), ("m", x_blk)):
            for w, near_w in (("g", g_near), ("u", u_near)):
                for j in range(2):
                    parts[w, s, j] = dot(near, near_w[j])

        def part(w, i, j):
            r = (i % CHUNKS) * rows
            return parts[w, "o" if i < CHUNKS else "m", j][r:r + rows]

        gates, hidden, hidden_far = {}, {}, {}
        for i in range(n):
            for j in range(2):
                gates[i, j] = (part("g", i, j) + dot(far[i], g_far[j])).astype(jnp.bfloat16)
                up = (part("u", i, j) + dot(far[i], u_far[j])).astype(jnp.bfloat16).astype(jnp.float32)
                gate = gates[i, j].astype(jnp.float32)
                hidden[i, j] = (jax.nn.silu(gate) * up).astype(jnp.bfloat16)
                hidden_far[i, j] = swap(hidden[i, j], "dy")

        z_from = []
        out = jnp.zeros(x_blk.shape, jnp.bfloat16)
        for i in range(n):
            pieces = [hidden[i, 0], hidden_far[i, 0], hidden[i, 1], hidden_far[i, 1]]
            z_part = dot(jnp.concatenate(pieces, axis=1), wd_perm)
            if i >= CHUNKS:
                z_part = (z_part + z_from[i - CHUNKS]).astype(jnp.bfloat16)
            if i < CHUNKS:
                z_from.append(swap(z_part, "dz"))
            else:
                out = lax.dynamic_update_slice(out, z_part, ((i - CHUNKS) * rows, 0))
        return out

    return jax.shard_map(body, mesh=mesh, in_specs=(x_spec, w_in_spec, w_in_spec, w_out_spec),
                         out_specs=x_spec, check_vma=False)
```

```python
import jax
import jax.numpy as jnp
from jax import lax
from jax.sharding import PartitionSpec as P


CHUNKS = 4


def solution(mesh):
    x_spec = P(("grp", "dx", "dz"), "dy")
    w_in_spec = P("dy", ("dz", "dx"))
    w_out_spec = P("dz", ("dy", "dx"))

    def swap(arr, axis):
        return lax.ppermute(arr, axis, [(0, 1), (1, 0)])

    def dot(lhs, rhs):
        return jnp.dot(lhs, rhs, preferred_element_type=jnp.float32)

    def body(x_blk, wg_blk, wu_blk, wd_blk):
        my_y = lax.axis_index("dy")
        my_c = lax.axis_index("dx")
        rows = x_blk.shape[0] // CHUNKS
        cols = wg_blk.shape[1] // 2
        n = 2 * CHUNKS

        def half(w_blk, which):
            return lax.dynamic_slice_in_dim(w_blk, which * cols, cols, axis=1)

        x_own = [x_blk[:rows]]
        x_rest, _ = lax.optimization_barrier((x_blk, x_own[0]))
        x_own += [x_rest[i * rows:(i + 1) * rows] for i in range(1, CHUNKS)]
        x_own_far = [swap(x_own[i], "dy") for i in range(CHUNKS)]
        x_oth = swap(x_blk, "dz")
        x_oth_far = [swap(x_own_far[i], "dz") for i in range(CHUNKS)]
        g_far = swap(half(wg_blk, 1 - my_y), "dy")
        u_far = swap(half(wu_blk, 1 - my_y), "dy")
        g_near = half(wg_blk, my_y)
        u_near = half(wu_blk, my_y)
        g_near = [g_near, swap(g_near, "dx")]
        u_near = [u_near, swap(u_near, "dx")]
        g_far = [g_far, swap(g_far, "dx")]
        u_far = [u_far, swap(u_far, "dx")]

        wd_other = swap(wd_blk, "dx")
        wd_all = jnp.where(my_c == 0, jnp.concatenate([wd_blk, wd_other], axis=1),
                           jnp.concatenate([wd_other, wd_blk], axis=1))
        wd4 = wd_all.reshape(2, 2, cols, wd_all.shape[1])
        wd4 = jnp.where(my_c == 1, lax.rev(wd4, (0,)), wd4)
        wd4 = jnp.where(my_y == 1, lax.rev(wd4, (1,)), wd4)
        wd_perm = wd4.reshape(wd_all.shape)

        far = x_oth_far + x_own_far
        parts = {}
        for s, near in (("o", x_oth), ("m", x_blk)):
            for w, near_w in (("g", g_near), ("u", u_near)):
                for j in range(2):
                    parts[w, s, j] = dot(near, near_w[j])

        def part(w, i, j):
            r = (i % CHUNKS) * rows
            return parts[w, "o" if i < CHUNKS else "m", j][r:r + rows]

        gates, hidden, hidden_far = {}, {}, {}
        for i in range(n):
            for j in range(2):
                gates[i, j] = (part("g", i, j) + dot(far[i], g_far[j])).astype(jnp.bfloat16)
                up = (part("u", i, j) + dot(far[i], u_far[j])).astype(jnp.bfloat16).astype(jnp.float32)
                gate = gates[i, j].astype(jnp.float32)
                hidden[i, j] = (jax.nn.silu(gate) * up).astype(jnp.bfloat16)
                if (i, j) == (n - 1, 1):
                    hidden_far[i, j] = [swap(hidden[i, j][k * rows // 2:(k + 1) * rows // 2], "dy")
                                        for k in range(2)]
                else:
                    hidden_far[i, j] = swap(hidden[i, j], "dy")

        z_from = []
        out = jnp.zeros(x_blk.shape, jnp.bfloat16)
        for i in range(n - 1):
            pieces = [hidden[i, 0], hidden_far[i, 0], hidden[i, 1], hidden_far[i, 1]]
            z_part = dot(jnp.concatenate(pieces, axis=1), wd_perm)
            if i >= CHUNKS:
                z_part = (z_part + z_from[i - CHUNKS]).astype(jnp.bfloat16)
            if i < CHUNKS:
                z_from.append(swap(z_part, "dz"))
            else:
                out = lax.dynamic_update_slice(out, z_part, ((i - CHUNKS) * rows, 0))
        i = n - 1
        z_part = dot(hidden[i, 1], wd_perm[2 * cols:3 * cols]) + z_from[CHUNKS - 1]
        z_part = dot(hidden[i, 0], wd_perm[:cols]) + z_part
        z_part = dot(hidden_far[i, 0], wd_perm[cols:2 * cols]) + z_part
        for k in range(2):
            z_half = dot(hidden_far[i, 1][k], wd_perm[3 * cols:]) + z_part[k * rows // 2:(k + 1) * rows // 2]
            z_half = z_half.astype(jnp.bfloat16)
            out = lax.dynamic_update_slice(out, z_half, ((CHUNKS - 1) * rows + k * rows // 2, 0))
        return out

    return jax.shard_map(body, mesh=mesh, in_specs=(x_spec, w_in_spec, w_in_spec, w_out_spec),
                         out_specs=x_spec, check_vma=False)
```

```python
import jax
import jax.numpy as jnp
from jax import lax
from jax.sharding import PartitionSpec as P


CHUNKS = 4


def solution(mesh):
    x_spec = P(("grp", "dx", "dz"), "dy")
    w_in_spec = P("dy", ("dz", "dx"))
    w_out_spec = P("dz", ("dy", "dx"))

    def swap(arr, axis):
        return lax.ppermute(arr, axis, [(0, 1), (1, 0)])

    def dot(lhs, rhs):
        return jnp.dot(lhs, rhs, preferred_element_type=jnp.float32)

    def body(x_blk, wg_blk, wu_blk, wd_blk):
        my_y = lax.axis_index("dy")
        my_c = lax.axis_index("dx")
        rows = x_blk.shape[0] // CHUNKS
        cols = wg_blk.shape[1] // 2
        n = 2 * CHUNKS

        def half(w_blk, which):
            return lax.dynamic_slice_in_dim(w_blk, which * cols, cols, axis=1)

        x_own = [x_blk[:rows]]
        x_rest, _ = lax.optimization_barrier((x_blk, x_own[0]))
        x_own += [x_rest[i * rows:(i + 1) * rows] for i in range(1, CHUNKS)]
        x_own_far = [swap(x_own[i], "dy") for i in range(CHUNKS)]
        x_oth = swap(x_blk, "dz")
        x_oth_far = [swap(x_own_far[i], "dz") for i in range(CHUNKS)]
        g_far = swap(half(wg_blk, 1 - my_y), "dy")
        u_far = swap(half(wu_blk, 1 - my_y), "dy")
        g_near = half(wg_blk, my_y)
        u_near = half(wu_blk, my_y)
        g_near = [g_near, swap(g_near, "dx")]
        u_near = [u_near, swap(u_near, "dx")]
        g_far = [g_far, swap(g_far, "dx")]
        u_far = [u_far, swap(u_far, "dx")]

        wd_other = swap(wd_blk, "dx")
        wd_all = jnp.where(my_c == 0, jnp.concatenate([wd_blk, wd_other], axis=1),
                           jnp.concatenate([wd_other, wd_blk], axis=1))
        wd4 = wd_all.reshape(2, 2, cols, wd_all.shape[1])
        wd4 = jnp.where(my_c == 1, lax.rev(wd4, (0,)), wd4)
        wd4 = jnp.where(my_y == 1, lax.rev(wd4, (1,)), wd4)
        wd_perm = wd4.reshape(wd_all.shape)

        far = x_oth_far + x_own_far
        parts = {}
        for s, near in (("o", x_oth), ("m", x_blk)):
            for w, near_w in (("g", g_near), ("u", u_near)):
                for j in range(2):
                    parts[w, s, j] = dot(near, near_w[j])

        def part(w, i, j):
            r = (i % CHUNKS) * rows
            return parts[w, "o" if i < CHUNKS else "m", j][r:r + rows]

        half_c, half_r = cols // 2, rows // 2
        tail = [(0, rows, 0, half_c), (0, rows, half_c, half_c + half_c // 2)]
        tail += [(k * half_r, (k + 1) * half_r, half_c + half_c // 2, cols) for k in range(2)]
        gates, hidden, hidden_far = {}, {}, {}
        for i in range(n):
            for j in range(2):
                gates[i, j] = (part("g", i, j) + dot(far[i], g_far[j])).astype(jnp.bfloat16)
                up = (part("u", i, j) + dot(far[i], u_far[j])).astype(jnp.bfloat16).astype(jnp.float32)
                gate = gates[i, j].astype(jnp.float32)
                hidden[i, j] = (jax.nn.silu(gate) * up).astype(jnp.bfloat16)
                if (i, j) == (n - 1, 1):
                    hidden_far[i, j] = [swap(hidden[i, j][r0:r1, c0:c1], "dy")
                                        for r0, r1, c0, c1 in tail]
                else:
                    hidden_far[i, j] = swap(hidden[i, j], "dy")

        z_from = []
        out = jnp.zeros(x_blk.shape, jnp.bfloat16)
        for i in range(n - 1):
            pieces = [hidden[i, 0], hidden_far[i, 0], hidden[i, 1], hidden_far[i, 1]]
            z_part = dot(jnp.concatenate(pieces, axis=1), wd_perm)
            if i >= CHUNKS:
                z_part = (z_part + z_from[i - CHUNKS]).astype(jnp.bfloat16)
            if i < CHUNKS:
                z_from.append(swap(z_part, "dz"))
            else:
                out = lax.dynamic_update_slice(out, z_part, ((i - CHUNKS) * rows, 0))
        i = n - 1
        z_part = dot(hidden[i, 1], wd_perm[2 * cols:3 * cols]) + z_from[CHUNKS - 1]
        z_part = lax.optimization_barrier(dot(hidden[i, 0], wd_perm[:cols]) + z_part)
        z_part = lax.optimization_barrier(dot(hidden_far[i, 0], wd_perm[cols:2 * cols]) + z_part)
        for k, (r0, r1, c0, c1) in enumerate(tail):
            z_piece = dot(hidden_far[i, 1][k], wd_perm[3 * cols + c0:3 * cols + c1]) + z_part[r0:r1]
            if c1 == cols:
                z_piece = z_piece.astype(jnp.bfloat16)
            if c1 == cols:
                out = lax.dynamic_update_slice(out, z_piece, ((CHUNKS - 1) * rows + r0, 0))
            else:
                z_part = z_piece
        return out

    return jax.shard_map(body, mesh=mesh, in_specs=(x_spec, w_in_spec, w_in_spec, w_out_spec),
                         out_specs=x_spec, check_vma=False)
```
